256 devices in a mesh: section: 2 (over z_hi), tile: 64 (over z_lo, y, x), member: 2 (over core).
Axes of the slice: x: 4, y: 4, z: 8 (z_hi: 2, z_lo: 4; z = z_hi * 4 + z_lo), core: 2. Of those that a mesh axis runs over, the one named last changes fastest.
Arguments:
- frames: bfloat16 [2, 128, 128, 8, 128], P(None, ('member', 'tile')), parts along dimension 1, may hold values from -6 to 6
- hidden_init: bfloat16 [4, 128, 128, 8, 128], P('section', ('member', 'tile')), parts along dimension 1, may hold values from -0.8984375 to 0.8984375
- memory_init: float32 [4, 128, 128, 8, 128], P('section', ('member', 'tile')), parts along dimension 1, may hold values from -4 to 4
- weights: bfloat16 [4, 512, 2304], P('section'), may hold values from -0.125 to 0.125
- biases: float32 [4, 512], P('section'), may hold values from -3 to 3
Outputs:
- hidden_out: bfloat16 [4, 128, 128, 8, 128], P('section', ('member', 'tile')), parts along dimension 1
- memory_out: float32 [4, 128, 128, 8, 128], P('section', ('member', 'tile')), parts along dimension 1
- gates_out: bfloat16 [2, 4, 128, 512, 8, 128], P(None, 'section', ('member', 'tile')), parts along dimension 2
The draws below stay inside these ranges and needn't reach their ends.
There are 2 independent parts, one for each index of `member`. The reference program is written for one: setup_inputs(seed, part) draws one part's arguments, and reference() takes and returns one part's arrays. A program takes and returns all parts, laid end to end along the dimension named above; an argument that names none is the same for every part. Nothing has to cross between parts.
All inputs are finite; a program needn't handle non-finite values.
Results may differ from the reference program's by a relative error of at most 0.0021.
Values may be sent and summed in bfloat16 or wider, within the bound.
A program may use at most 128 MiB of HBM per device.

```python
import jax
import jax.numpy as jnp

HID = 128
TILE_ROWS = 8
TILE_COLS = 128
GRID_COLS = 8
STEPS = 2
TILES = 64
LAYERS = 4


def block_levels(rng, extent, pieces, smallest, top_value):
    def one(dim, blocks):
        steps = jax.random.uniform(jax.random.fold_in(jax.random.fold_in(rng, 6), dim), (blocks,), jnp.float32, smallest / len(pieces), top_value / len(pieces))
        return jnp.repeat(jnp.exp(steps), extent[dim] // blocks).reshape((-1,) + (1,) * (len(extent) - dim - 1))

    gain = one(*pieces[0])
    for cut in pieces[1:]:
        gain = gain * one(*cut)
    return gain


def scatter_about(rng, shape, deviation, bound, pieces=(), dtype=jnp.bfloat16):
    result = jax.random.normal(rng, shape, jnp.float32) * deviation
    if len(pieces) > 0:
        result = block_levels(rng, shape, pieces, -0.22, 0.18) * result
    return jnp.clip(result, min=-bound, max=bound).astype(dtype)


def setup_inputs(seed: int = 0, part: int = 0) -> dict:
    arg_keys = jax.random.split(jax.random.key(seed), 6)
    part_splits = jax.random.split(jax.random.fold_in(arg_keys[5], part), 6)
    return {
        "frames": scatter_about(part_splits[0], (STEPS, TILES, HID, TILE_ROWS, TILE_COLS), 1.0, 6.0, ((1, 64),)),
        "hidden_init": jnp.clip(jax.random.uniform(part_splits[1], (LAYERS, TILES, HID, TILE_ROWS, TILE_COLS), jnp.float32, -0.8984375, 0.8984375) * block_levels(part_splits[1], (LAYERS, TILES, HID, TILE_ROWS, TILE_COLS), ((0, 2), (1, 64)), -0.4, 0.0), -0.8984375, 0.8984375).astype(jnp.bfloat16),
        "memory_init": scatter_about(part_splits[2], (LAYERS, TILES, HID, TILE_ROWS, TILE_COLS), 1.0, 4.0, ((0, 2), (1, 64)), jnp.float32),
        "weights": scatter_about(arg_keys[3], (LAYERS, 4 * HID, 18 * HID), (18 * HID) ** -0.5, 0.125, ((0, 2),)),
        "biases": scatter_about(arg_keys[4], (LAYERS, 4 * HID), 0.5, 3.0, ((0, 2),), jnp.float32),
    }


def to_frame(tile_array):
    tile_count, depth_count, height, breadth = tile_array.shape
    grid_rows = tile_count // GRID_COLS
    placed = jnp.roll(tile_array, GRID_COLS + GRID_COLS // 2, axis=0)
    shaped = placed.reshape(grid_rows, GRID_COLS, depth_count, height, breadth)
    return shaped.transpose(2, 0, 3, 1, 4).reshape(depth_count, grid_rows * height, GRID_COLS * breadth)


def to_tiles(full_field):
    depth_count = full_field.shape[0]
    grid_rows = full_field.shape[1] // TILE_ROWS
    shaped = full_field.reshape(depth_count, grid_rows, TILE_ROWS, GRID_COLS, TILE_COLS)
    placed = shaped.transpose(1, 3, 0, 2, 4).reshape(grid_rows * GRID_COLS, depth_count, TILE_ROWS, TILE_COLS)
    return jnp.roll(placed, -(GRID_COLS + GRID_COLS // 2), axis=0)


def gate_inputs(stacked, layer_weights, bias_row):
    depth_count, height, breadth = stacked.shape
    padded = jnp.pad(stacked, ((0, 0), (1, 1), (1, 1)))
    running_total = jnp.zeros((layer_weights.shape[0], height * breadth), jnp.float32)
    for offset in range(9):
        row_offset = offset // 3
        column_offset = offset % 3
        window = padded[:, row_offset:row_offset + height, column_offset:column_offset + breadth].reshape(depth_count, height * breadth)
        kernel = layer_weights[:, offset * depth_count:(offset + 1) * depth_count]
        running_total = running_total + jnp.dot(kernel, window, preferred_element_type=jnp.float32)
    running_total = running_total + bias_row[:, None]
    return running_total.reshape(4, layer_weights.shape[0] // 4, height, breadth)


def reference(frames, hidden_init, memory_init, weights, biases):
    states = [to_frame(hidden_init[layer_index]) for layer_index in range(LAYERS)]
    memories = [to_frame(memory_init[layer_index]) for layer_index in range(LAYERS)]
    saved_gates = []
    for moment in range(STEPS):
        sources = [to_frame(frames[moment])] + states[:-1]
        fresh_states = []
        fresh_memories = []
        opened_step = []
        for layer_index in range(LAYERS):
            stacked = jnp.concatenate([sources[layer_index], states[layer_index]], axis=0)
            preact = gate_inputs(stacked, weights[layer_index], biases[layer_index])
            inflow = jax.nn.sigmoid(preact[0])
            forget = jax.nn.sigmoid(preact[1])
            outflow = jax.nn.sigmoid(preact[2])
            candidate = jnp.tanh(preact[3])
            memory = forget * memories[layer_index] + inflow * candidate
            hidden_state = (outflow * jnp.tanh(memory)).astype(jnp.bfloat16)
            opened = jnp.concatenate([inflow, forget, outflow, candidate], axis=0).astype(jnp.bfloat16)
            fresh_states.append(hidden_state)
            fresh_memories.append(memory)
            opened_step.append(to_tiles(opened))
        states = fresh_states
        memories = fresh_memories
        saved_gates.append(jnp.stack(opened_step))
    hidden_out = jnp.stack([to_tiles(item) for item in states])
    memory_out = jnp.stack([to_tiles(item) for item in memories])
    return (hidden_out, memory_out, jnp.stack(saved_gates))
```

```python
import jax
import jax.numpy as jnp
from jax import lax
from jax.experimental import pallas as pl
from jax.experimental.pallas import tpu as pltpu
from jax.sharding import PartitionSpec as P

GRID_COLS = 8
MESH = pl.DeviceIdType.MESH
F32 = jnp.float32
BF16 = jnp.bfloat16

ROW_UP, ROW_DOWN = 0, 1
NEIGHBOURS = (-8, 8, 1, 9, -7, -1, 7, -9)
BULK = 2


def sigmoid(x):
    return 0.5 * jnp.tanh(0.5 * x) + 0.5


def kernel(
    frames, hidden, memory, weights, biases,
    hidden_out, memory_out, gates_out,
    patch, spread, hidden_raw, frames_raw, cell, weight, bias_rows, bias,
    gate_wide, gate_narrow, hidden_narrow, edge_send, edge_recv,
    load_sem, store_sem, send_sem, recv_sem, bulk_send, bulk_recv,
):
    section = lax.axis_index("section")
    tile = lax.axis_index("tile")
    member = lax.axis_index("member")
    tiles = lax.axis_size("tile")
    place = lax.rem(tile + GRID_COLS + GRID_COLS // 2, tiles)
    grid_row, grid_col = place // GRID_COLS, lax.rem(place, GRID_COLS)
    has_up, has_down = grid_row > 0, grid_row < tiles // GRID_COLS - 1
    has_left, has_right = grid_col > 0, grid_col < GRID_COLS - 1

    def device(which, distance):
        return (which, lax.rem(tile + distance + tiles, tiles), member)

    loads = [
        pltpu.make_async_copy(hidden, hidden_raw, load_sem.at[0]),
        pltpu.make_async_copy(frames, frames_raw, load_sem.at[1]),
        pltpu.make_async_copy(biases, bias_rows, load_sem.at[2]),
        pltpu.make_async_copy(weights.at[1], weight.at[1], load_sem.at[3]),
        pltpu.make_async_copy(memory, cell, load_sem.at[4]),
        pltpu.make_async_copy(weights.at[0], weight.at[0], load_sem.at[5]),
    ]
    for load in loads:
        load.start()

    barrier = pltpu.get_barrier_semaphore()
    for distance in NEIGHBOURS:
        pl.semaphore_signal(barrier, 1, device_id=device(section, distance), device_id_type=MESH)
    for distance in (0,) + NEIGHBOURS:
        pl.semaphore_signal(barrier, 1, device_id=device(1 - section, distance), device_id_type=MESH)

    def slot(index):
        return pl.ds(index * 128, 128)

    def message(step, source, target, flow, which, number):
        if number == ROW_UP:
            src = patch.at[step, 1, 1, slot(source)]
            dst = patch.at[step, 1, 9, slot(target)]
        elif number == ROW_DOWN:
            src = patch.at[step, 1, 8, slot(source)]
            dst = patch.at[step, 1, 0, slot(target)]
        else:
            src = edge_send.at[step, source, 0 if number < 5 else 1]
            dst = edge_recv.at[step, target, number - 2]
        return pltpu.make_async_remote_copy(
            src_ref=src, dst_ref=dst,
            send_sem=send_sem.at[step, flow, number], recv_sem=recv_sem.at[step, target, number],
            device_id=device(which, NEIGHBOURS[number]), device_id_type=MESH,
        )

    def messages(step, source, target, flow, which):
        return [message(step, source, target, flow, which, n) for n in range(8)]

    def bulk(step):
        rows = 8 // BULK
        return [
            pltpu.make_async_remote_copy(
                src_ref=patch.at[step, 1, pl.ds(1 + n * rows, rows), slot(2)],
                dst_ref=patch.at[step, 1, pl.ds(1 + n * rows, rows), slot(0)],
                send_sem=bulk_send.at[step, n], recv_sem=bulk_recv.at[step, n],
                device_id=device(1, 0), device_id_type=MESH,
            )
            for n in range(BULK)
        ]

    def lay_out(raw, step, index):
        spread[...] = raw.astype(F32)
        for y in range(8):
            patch[step, 1, 1 + y, slot(index), :] = spread[pl.ds(y, 128, stride=8), :].astype(BF16)

    row_of = lax.broadcasted_iota(jnp.int32, (16, 128), 0)
    lane_of = lax.broadcasted_iota(jnp.int32, (16, 128), 1)

    def take_edges(step, index):
        left = jnp.zeros((16, 128), F32)
        right = jnp.zeros((16, 128), F32)
        for y in range(8):
            pick = jnp.concatenate(
                [((row_of == y) & (lane_of == 0)).astype(F32), ((row_of == y) & (lane_of == 127)).astype(F32)], axis=0
            ).astype(BF16)
            both = lax.dot_general(
                pick, patch[step, 1, 1 + y, slot(index), :], (((1,), (1,)), ((), ())), preferred_element_type=F32
            )
            left += both[:16]
            right += both[16:]
        edge_send[step, index, 0] = right.astype(BF16)
        edge_send[step, index, 1] = left.astype(BF16)

    lane = lax.broadcasted_iota(jnp.int32, (128, 128), 1)

    def insert(step, index):
        edges = edge_recv[step, index].reshape(96, 128).astype(F32)
        edges = jnp.concatenate([edges, jnp.zeros((32, 128), F32)], axis=0).T

        def one_row(r, left_at, right_at, live):
            x = patch[step, 1, r, slot(index), :].astype(F32)
            if live is not None:
                x = jnp.where(live, x, 0.0)
                patch[step, 1, r, slot(index), :] = x.astype(BF16)
            from_left = jnp.where(has_left if live is None else live & has_left, pltpu.roll(edges, 128 - left_at, 1), 0.0)
            from_right = jnp.where(has_right if live is None else live & has_right, pltpu.roll(edges, 127 - right_at, 1), 0.0)
            patch[step, 0, r, slot(index), :] = jnp.where(lane == 0, from_left, pltpu.roll(x, 1, 1)).astype(BF16)
            patch[step, 2, r, slot(index), :] = jnp.where(lane == 127, from_right, pltpu.roll(x, 127, 1)).astype(BF16)

        def inner_row(r, carry):
            one_row(r, r - 1, r + 47, None)
            return carry

        one_row(0, 23, 71, has_up)
        one_row(9, 32, 80, has_down)
        lax.fori_loop(1, 9, inner_row, 0)

    def layer(step, index):
        width = pl.ds(index * 128, 256)

        def two_rows(pair, carry):
            acc = None
            for a in range(3):
                for b in range(3):
                    rhs = jnp.concatenate(
                        [patch[step, b, 2 * pair + r + a, width, :] for r in range(2)], axis=1
                    )
                    tap = a * 3 + b
                    part = jnp.dot(weight[index, :, tap * 256:(tap + 1) * 256], rhs, preferred_element_type=F32)
                    acc = part if acc is None else acc + part
            for r in range(2):
                y = 2 * pair + r
                pre = acc[:, r * 128:(r + 1) * 128] + bias[index]
                inflow = sigmoid(pre[0:128])
                forget = sigmoid(pre[128:256])
                outflow = sigmoid(pre[256:384])
                candidate = jnp.tanh(pre[384:512])
                for n, gate in enumerate((inflow, forget, outflow, candidate)):
                    gate_wide[pl.ds(y + n * 1024, 128, stride=8), :] = gate
                old = cell[index, pl.ds(y, 128, stride=8), :]
                new = forget * old + inflow * candidate
                cell[index, pl.ds(y, 128, stride=8), :] = new
                state = outflow * jnp.tanh(new)
                if step == 0:
                    patch[1, 1, 1 + y, slot(1 + index), :] = state.astype(BF16)
                else:
                    spread[pl.ds(y, 128, stride=8), :] = state
            return carry

        lax.fori_loop(0, 4, two_rows, 0)

        def narrow(n, carry):
            rows = pl.ds(pl.multiple_of(n * 256, 256), 256)
            gate_narrow[step, index, rows, :] = gate_wide[rows, :].astype(BF16)
            return carry

        lax.fori_loop(0, 16, narrow, 0)
        stores[step, index].start()
        if step == 1:
            hidden_narrow[index] = spread[...].astype(BF16)
            stores["hidden", index].start()
            stores["memory", index].start()

    stores = {}
    for step in range(2):
        for index in range(2):
            stores[step, index] = pltpu.make_async_copy(
                gate_narrow.at[step, index], gates_out.at[step, index], store_sem.at[step * 2 + index]
            )
    for index in range(2):
        stores["hidden", index] = pltpu.make_async_copy(
            hidden_narrow.at[index], hidden_out.at[index], store_sem.at[4 + index]
        )
        stores["memory", index] = pltpu.make_async_copy(cell.at[index], memory_out.at[index], store_sem.at[6 + index])

    def start(copies):
        for copy in copies:
            copy.start()

    def wait_recv(copies):
        for copy in copies:
            copy.wait_recv()

    loads[0].wait()
    for index in range(2):
        lay_out(hidden_raw[index], 0, 1 + index)
        take_edges(0, 1 + index)
    pl.semaphore_wait(barrier, 17)
    start(messages(0, 2, 2, 2, section))
    start(messages(0, 1, 1, 1, section))

    @pl.when(section == 0)
    def _():
        start(bulk(0))
        start(messages(0, 2, 0, 3, 1))

    loads[1].wait()

    @pl.when(section == 0)
    def _():
        for step in range(2):
            lay_out(frames_raw[step], step, 0)
            take_edges(step, 0)
            start(messages(step, 0, 0, 0, 0))

    loads[2].wait()
    rows = jnp.concatenate([bias_rows[n // 4:n // 4 + 1, (n % 4) * 128:(n % 4 + 1) * 128] for n in range(8)], axis=0)
    columns = jnp.concatenate([rows, jnp.zeros((120, 128), F32)], axis=0).T
    for n in range(8):
        bias[n // 4, (n % 4) * 128:(n % 4 + 1) * 128, :] = jnp.broadcast_to(columns[:, n:n + 1], (128, 128))

    for step in range(2):
        for index in (2, 1):
            wait_recv(messages(step, index, index, index, section))
            insert(step, index)
        if step == 0:
            for n in (3, 4, 5):
                loads[n].wait()
        layer(step, 1)
        if step == 0:
            take_edges(1, 2)

            @pl.when(section == 0)
            def _():
                start(bulk(1))
                start(messages(1, 2, 0, 3, 1))

            start(messages(1, 2, 2, 2, section))

        @pl.when(section == 1)
        def _():
            wait_recv(bulk(step))

        wait_recv(messages(step, 0, 0, 0, 0))
        insert(step, 0)
        layer(step, 0)
        if step == 0:
            take_edges(1, 1)
            start(messages(1, 1, 1, 1, section))

    for step in range(2):
        for index in (1, 2):
            for copy in messages(step, index, index, index, section):
                copy.wait_send()

    @pl.when(section == 0)
    def _():
        for step in range(2):
            for copy in bulk(step) + messages(step, 0, 0, 0, 0) + messages(step, 2, 0, 3, 1):
                copy.wait_send()

    for copy in stores.values():
        copy.wait()


def body(frames, hidden_init, memory_init, weights, biases):
    frames = frames.reshape(2, 1024, 128)
    hidden_init = hidden_init.reshape(2, 1024, 128)
    memory_init = memory_init.reshape(2, 1024, 128)
    vmem = pltpu.VMEM
    dma = pltpu.SemaphoreType.DMA
    hidden_out, memory_out, gates_out = pl.pallas_call(
        kernel,
        out_shape=(
            jax.ShapeDtypeStruct((2, 1024, 128), BF16),
            jax.ShapeDtypeStruct((2, 1024, 128), F32),
            jax.ShapeDtypeStruct((2, 2, 4096, 128), BF16),
        ),
        in_specs=[pl.BlockSpec(memory_space=pl.ANY)] * 5,
        out_specs=[pl.BlockSpec(memory_space=pl.ANY)] * 3,
        scratch_shapes=[
            vmem((2, 3, 10, 384, 128), BF16),
            vmem((1024, 128), F32),
            vmem((2, 1024, 128), BF16),
            vmem((2, 1024, 128), BF16),
            vmem((2, 1024, 128), F32),
            vmem((2, 512, 2304), BF16),
            vmem((2, 512), F32),
            vmem((2, 512, 128), F32),
            vmem((4096, 128), F32),
            vmem((2, 2, 4096, 128), BF16),
            vmem((2, 1024, 128), BF16),
            vmem((2, 3, 2, 16, 128), BF16),
            vmem((2, 3, 6, 16, 128), BF16),
            dma((6,)),
            dma((8,)),
            dma((2, 4, 8)),
            dma((2, 3, 8)),
            dma((2, BULK)),
            dma((2, BULK)),
        ],
        compiler_params=pltpu.CompilerParams(
            collective_id=0, has_side_effects=True, vmem_limit_bytes=56 << 20
        ),
        name="wavefront",
    )(frames, hidden_init, memory_init, weights, biases)
    return (
        hidden_out.reshape(2, 1, 128, 8, 128),
        memory_out.reshape(2, 1, 128, 8, 128),
        gates_out.reshape(2, 2, 1, 512, 8, 128),
    )


def solution(mesh):
    states = P("section", ("member", "tile"), None, None, None)
    in_specs = (
        P(None, ("member", "tile"), None, None, None),
        states,
        states,
        P("section", None, None),
        P("section", None),
    )
    out_specs = (states, states, P(None, "section", ("member", "tile"), None, None, None))
    return jax.shard_map(body, mesh=mesh, in_specs=in_specs, out_specs=out_specs, check_vma=False)
```

```python
import contextlib

import jax
import jax.numpy as jnp
from jax import lax
from jax.experimental import pallas as pl
from jax.experimental.pallas import tpu as pltpu
from jax.sharding import PartitionSpec as P

GRID_COLS = 8
MESH = pl.DeviceIdType.MESH
F32 = jnp.float32
BF16 = jnp.bfloat16

ROW_UP, ROW_DOWN = 0, 1
NEIGHBOURS = (-8, 8, 1, 9, -7, -1, 7, -9)
UNROLL = 4
CROSS = tuple((row, 1) for row in (1, 8, 2, 3, 4, 5, 6, 7))


def phase(name):
    return contextlib.nullcontext()


def sigmoid(x):
    return 0.5 * jnp.tanh(0.5 * x) + 0.5


def kernel(
    frames, hidden, memory, weights, biases,
    hidden_narrow, cell, gate_narrow,
    patch, spread, hidden_raw, frames_raw, weight, bias_rows, bias,
    gate_wide, partial, edge_send, edge_recv,
    load_sem, send_sem, recv_sem, cross_send, cross_recv,
):
    section = lax.axis_index("section")
    tile = lax.axis_index("tile")
    member = lax.axis_index("member")
    tiles = lax.axis_size("tile")
    place = lax.rem(tile + GRID_COLS + GRID_COLS // 2, tiles)
    grid_row, grid_col = place // GRID_COLS, lax.rem(place, GRID_COLS)
    has_up, has_down = grid_row > 0, grid_row < tiles // GRID_COLS - 1
    has_left, has_right = grid_col > 0, grid_col < GRID_COLS - 1

    def device(which, distance):
        return (which, lax.rem(tile + distance + tiles, tiles), member)

    loads = [
        pltpu.make_async_copy(hidden, hidden_raw, load_sem.at[0]),
        pltpu.make_async_copy(frames, frames_raw, load_sem.at[1]),
        pltpu.make_async_copy(biases, bias_rows, load_sem.at[2]),
        pltpu.make_async_copy(weights.at[1], weight.at[1], load_sem.at[3]),
        pltpu.make_async_copy(memory, cell, load_sem.at[4]),
        pltpu.make_async_copy(weights.at[0], weight.at[0], load_sem.at[5]),
    ]
    for load in loads:
        load.start()

    barrier = pltpu.get_barrier_semaphore()
    for distance in NEIGHBOURS:
        pl.semaphore_signal(barrier, 1, device_id=device(section, distance), device_id_type=MESH)
    pl.semaphore_signal(barrier, 1, device_id=device(1 - section, 0), device_id_type=MESH)

    def slot(index):
        return pl.ds(index * 128, 128)

    def message(step, source, target, flow, which, number):
        if number == ROW_UP:
            src = patch.at[step, 1, 1, slot(source)]
            dst = patch.at[step, 1, 9, slot(target)]
        elif number == ROW_DOWN:
            src = patch.at[step, 1, 8, slot(source)]
            dst = patch.at[step, 1, 0, slot(target)]
        else:
            src = edge_send.at[step, source, 0 if number < 5 else 1]
            dst = edge_recv.at[step, target, number - 2]
        return pltpu.make_async_remote_copy(
            src_ref=src, dst_ref=dst,
            send_sem=send_sem.at[step, flow, number], recv_sem=recv_sem.at[step, target, number],
            device_id=device(which, NEIGHBOURS[number]), device_id_type=MESH,
        )

    def messages(step, source, target, flow, which):
        return [message(step, source, target, flow, which, n) for n in range(8)]

    def cross(step):
        copies = [(edge_send.at[step, 2], edge_send.at[step, 0])]
        for first, count in CROSS:
            rows = pl.ds(first, count)
            copies.append((patch.at[step, 1, rows, slot(2)], patch.at[step, 1, rows, slot(0)]))
        return [
            pltpu.make_async_remote_copy(
                src_ref=src, dst_ref=dst, send_sem=cross_send.at[step, n], recv_sem=cross_recv.at[step, n],
                device_id=device(1, 0), device_id_type=MESH,
            )
            for n, (src, dst) in enumerate(copies)
        ]

    def lay_out(raw, step, index):
        spread[...] = raw.astype(F32)
        for y in range(8):
            patch[step, 1, 1 + y, slot(index), :] = spread[pl.ds(y, 128, stride=8), :].astype(BF16)

    row_of = lax.broadcasted_iota(jnp.int32, (16, 128), 0)
    lane_of = lax.broadcasted_iota(jnp.int32, (16, 128), 1)

    def take_edges(step, index):
        left = jnp.zeros((16, 128), F32)
        right = jnp.zeros((16, 128), F32)
        for y in range(8):
            pick = jnp.concatenate(
                [((row_of == y) & (lane_of == 0)).astype(F32), ((row_of == y) & (lane_of == 127)).astype(F32)], axis=0
            ).astype(BF16)
            both = lax.dot_general(
                pick, patch[step, 1, 1 + y, slot(index), :], (((1,), (1,)), ((), ())), preferred_element_type=F32
            )
            left += both[:16]
            right += both[16:]
        edge_send[step, index, 0] = right.astype(BF16)
        edge_send[step, index, 1] = left.astype(BF16)

    lane = lax.broadcasted_iota(jnp.int32, (128, 128), 1)

    def insert(step, index):
        edges = edge_recv[step, index].reshape(96, 128).astype(F32)
        edges = jnp.concatenate([edges, jnp.zeros((32, 128), F32)], axis=0).T

        def one_row(r, left_at, right_at, live):
            x = patch[step, 1, r, slot(index), :].astype(F32)
            if live is not None:
                x = jnp.where(live, x, 0.0)
                patch[step, 1, r, slot(index), :] = x.astype(BF16)
            from_left = jnp.where(has_left if live is None else live & has_left, pltpu.roll(edges, 128 - left_at, 1), 0.0)
            from_right = jnp.where(has_right if live is None else live & has_right, pltpu.roll(edges, 127 - right_at, 1), 0.0)
            patch[step, 0, r, slot(index), :] = jnp.where(lane == 0, from_left, pltpu.roll(x, 1, 1)).astype(BF16)
            patch[step, 2, r, slot(index), :] = jnp.where(lane == 127, from_right, pltpu.roll(x, 127, 1)).astype(BF16)

        def inner_row(r, carry):
            one_row(r, r - 1, r + 47, None)
            return carry

        one_row(0, 23, 71, has_up)
        one_row(9, 32, 80, has_down)
        lax.fori_loop(1, 9, inner_row, 0, unroll=4)

    def product(step, index, pair, parts):
        chunks = [(tap, part) for tap in range(9) for part in parts]
        acc = None
        for first in range(0, len(chunks), 2):
            group = chunks[first:first + 2]
            lhs = jnp.concatenate(
                [weight[index, :, tap * 256 + part * 128:tap * 256 + part * 128 + 128] for tap, part in group], axis=1
            )
            rhs = jnp.concatenate(
                [
                    jnp.concatenate(
                        [patch[step, tap % 3, 2 * pair + r + tap // 3, slot(index + part), :] for r in range(2)], axis=1
                    )
                    for tap, part in group
                ],
                axis=0,
            )
            dot = jnp.dot(lhs, rhs, preferred_element_type=F32)
            acc = dot if acc is None else acc + dot
        return acc

    def first_half(step, index):
        def two_rows(pair, carry):
            offset = jnp.concatenate([bias[index]] * 2, axis=1)
            partial[pair] = product(step, index, pair, (1,)) + offset
            return carry

        lax.fori_loop(0, 4, two_rows, 0, unroll=UNROLL)

    def layer(step, index, whole):
        def two_rows(pair, carry):
            if whole:
                acc = product(step, index, pair, (0, 1)) + jnp.concatenate([bias[index]] * 2, axis=1)
            else:
                acc = product(step, index, pair, (0,)) + partial[pair]
            for r in range(2):
                y = 2 * pair + r
                pre = acc[:, r * 128:(r + 1) * 128]
                inflow = sigmoid(pre[0:128])
                forget = sigmoid(pre[128:256])
                outflow = sigmoid(pre[256:384])
                candidate = jnp.tanh(pre[384:512])
                for n, gate in enumerate((inflow, forget, outflow, candidate)):
                    gate_wide[pl.ds(y + n * 1024, 128, stride=8), :] = gate
                old = cell[index, pl.ds(y, 128, stride=8), :]
                new = forget * old + inflow * candidate
                cell[index, pl.ds(y, 128, stride=8), :] = new
                state = outflow * jnp.tanh(new)
                if step == 0:
                    patch[1, 1, 1 + y, slot(1 + index), :] = state.astype(BF16)
                else:
                    spread[pl.ds(y, 128, stride=8), :] = state
            return carry

        lax.fori_loop(0, 4, two_rows, 0, unroll=UNROLL)

    def finish(step, index):
        def narrow(n, carry):
            rows = pl.ds(pl.multiple_of(n * 256, 256), 256)
            gate_narrow[step, index, rows, :] = gate_wide[rows, :].astype(BF16)
            return carry

        lax.fori_loop(0, 16, narrow, 0, unroll=4)
        if step == 1:
            hidden_narrow[index] = spread[...].astype(BF16)

    def start(copies):
        for copy in copies:
            copy.start()

    def wait_recv(copies):
        for copy in copies:
            copy.wait_recv()

    def wait_send(copies):
        for copy in copies:
            copy.wait_send()

    def on(which, action):
        pl.when(section == which)(action)

    with phase("load"):
        loads[0].wait()
    with phase("lay"):
        for index in range(2):
            lay_out(hidden_raw[index], 0, 1 + index)
            take_edges(0, 1 + index)
    with phase("framesprep"):
        loads[1].wait()

        @pl.when(section == 0)
        def _():
            for step in range(2):
                lay_out(frames_raw[step], step, 0)
                take_edges(step, 0)

    with phase("barrier"):
        pl.semaphore_wait(barrier, 9)
    with phase("send0"):
        start(messages(0, 2, 2, 2, section))
        start(messages(0, 1, 1, 1, section))

        @pl.when(section == 0)
        def _():
            start(messages(0, 0, 0, 0, section))
            start(cross(0))

    with phase("bias"):
        loads[2].wait()
        rows = jnp.concatenate([bias_rows[n // 4:n // 4 + 1, (n % 4) * 128:(n % 4 + 1) * 128] for n in range(8)], axis=0)
        columns = jnp.concatenate([rows, jnp.zeros((120, 128), F32)], axis=0).T
        for n in range(8):
            bias[n // 4, (n % 4) * 128:(n % 4 + 1) * 128, :] = jnp.broadcast_to(columns[:, n:n + 1], (128, 128))

    depth = tile // 16
    inner = (depth == 1) | (depth == 2)

    def take_in(step, index, first=0):
        with phase(f"wait_halo_s{step}_{index}"):
            wait_recv(messages(step, index, index, index, section)[first:])
        with phase(f"insert_s{step}_{index}"):
            insert(step, index)

    def pass_on(step):
        with phase(f"pass_on_s{step}"):
            @pl.when(section == 1)
            def _():
                wait_recv(cross(step)[:3])
                start(messages(step, 0, 0, 0, section))

    def rest(step):
        with phase(f"wait_rest_s{step}"):
            @pl.when(section == 1)
            def _():
                wait_recv(cross(step)[3:])

    take_in(0, 2)
    take_in(0, 1)
    with phase("wait_w"):
        for n in (3, 4, 5):
            loads[n].wait()
    with phase("layer_s0_1"):
        layer(0, 1, True)
    with phase("send1"):
        start(messages(1, 2, 2, 2, section)[:2])
        take_edges(1, 2)
        start(messages(1, 2, 2, 2, section)[2:])

        @pl.when((section == 0) & inner)
        def _():
            start(cross(1))

        @pl.when(section == 0)
        def _():
            start(messages(1, 0, 0, 0, section))

    pass_on(0)
    with phase("finish_s0_1"):
        finish(0, 1)
    with phase("half_s0_0"):
        first_half(0, 0)
    rest(0)
    take_in(0, 0)
    with phase("layer_s0_0"):
        layer(0, 0, False)
    with phase("send2"):
        start(messages(1, 1, 1, 1, section)[:2])
        take_edges(1, 1)
        start(messages(1, 1, 1, 1, section)[2:])

    with phase("finish_s0_0"):
        finish(0, 0)
    take_in(1, 2)
    with phase("half_s1_1"):
        first_half(1, 1)

    @pl.when((section == 0) & jnp.logical_not(inner))
    def _():
        start(cross(1))

    pass_on(1)
    take_in(1, 1)
    with phase("layer_s1_1"):
        layer(1, 1, False)
    with phase("finish_s1_1"):
        finish(1, 1)
    with phase("half_s1_0"):
        first_half(1, 0)
    rest(1)
    take_in(1, 0)
    with phase("layer_s1_0"):
        layer(1, 0, False)
    with phase("finish_s1_0"):
        finish(1, 0)

    for step in range(2):
        for index in range(3):
            wait_send(messages(step, index, index, index, section))

    @pl.when(section == 0)
    def _():
        for step in range(2):
            wait_send(cross(step))


def write_out(*refs):
    sources, targets, sem = refs[:3], refs[3:6], refs[6]
    copies = [pltpu.make_async_copy(src, dst, sem.at[n]) for n, (src, dst) in enumerate(zip(sources, targets))]
    for copy in copies:
        copy.start()
    for copy in copies:
        copy.wait()


def body(frames, hidden_init, memory_init, weights, biases):
    frames = frames.reshape(2, 1024, 128)
    hidden_init = hidden_init.reshape(2, 1024, 128)
    memory_init = memory_init.reshape(2, 1024, 128)
    vmem = pltpu.VMEM
    dma = pltpu.SemaphoreType.DMA
    shapes = (
        jax.ShapeDtypeStruct((2, 1024, 128), BF16),
        jax.ShapeDtypeStruct((2, 1024, 128), F32),
        jax.ShapeDtypeStruct((2, 2, 4096, 128), BF16),
    )
    results = pl.pallas_call(
        kernel,
        out_shape=shapes,
        in_specs=[pl.BlockSpec(memory_space=pltpu.HBM)] * 5,
        out_specs=[pl.BlockSpec(memory_space=pltpu.VMEM)] * 3,
        scratch_shapes=[
            vmem((2, 3, 10, 384, 128), BF16),
            vmem((1024, 128), F32),
            vmem((2, 1024, 128), BF16),
            vmem((2, 1024, 128), BF16),
            vmem((2, 512, 2304), BF16),
            vmem((2, 512), F32),
            vmem((2, 512, 128), F32),
            vmem((4096, 128), F32),
            vmem((4, 512, 256), F32),
            vmem((2, 3, 2, 16, 128), BF16),
            vmem((2, 3, 6, 16, 128), BF16),
            dma((6,)),
            dma((2, 3, 8)),
            dma((2, 3, 8)),
            dma((2, 1 + len(CROSS))),
            dma((2, 1 + len(CROSS))),
        ],
        compiler_params=pltpu.CompilerParams(
            collective_id=0, has_side_effects=True, vmem_limit_bytes=32 << 20
        ),
        name="wavefront",
    )(*[pltpu.with_memory_space_constraint(x, pltpu.HBM) for x in (frames, hidden_init, memory_init, weights, biases)])
    hidden_out, memory_out, gates_out = pl.pallas_call(
        write_out,
        out_shape=shapes,
        in_specs=[pl.BlockSpec(memory_space=pl.ANY)] * 3,
        out_specs=[pl.BlockSpec(memory_space=pltpu.HBM)] * 3,
        scratch_shapes=[dma((3,))],
        compiler_params=pltpu.CompilerParams(vmem_limit_bytes=1 << 20),
        name="write_out",
    )(*results)
    return (
        hidden_out.reshape(2, 1, 128, 8, 128),
        memory_out.reshape(2, 1, 128, 8, 128),
        gates_out.reshape(2, 2, 1, 512, 8, 128),
    )


def solution(mesh):
    states = P("section", ("member", "tile"), None, None, None)
    in_specs = (
        P(None, ("member", "tile"), None, None, None),
        states,
        states,
        P("section", None, None),
        P("section", None),
    )
    out_specs = (states, states, P(None, "section", ("member", "tile"), None, None, None))
    return jax.shard_map(body, mesh=mesh, in_specs=in_specs, out_specs=out_specs, check_vma=False)
```

```python
import contextlib

import jax
import jax.numpy as jnp
from jax import lax
from jax.experimental import pallas as pl
from jax.experimental.pallas import tpu as pltpu
from jax.sharding import PartitionSpec as P

GRID_COLS = 8
MESH = pl.DeviceIdType.MESH
F32 = jnp.float32
BF16 = jnp.bfloat16

ROW_UP, ROW_DOWN = 0, 1
NEIGHBOURS = (-8, 8, 1, 9, -7, -1, 7, -9)
CROSS = tuple((row, 1) for row in (1, 8, 2, 3, 4, 5, 6, 7))


def phase(name):
    return contextlib.nullcontext()


def sigmoid(x):
    return 0.5 * jnp.tanh(0.5 * x) + 0.5


def kernel(
    frames, hidden, memory, weights, biases,
    hidden_narrow, cell, gate_narrow,
    patch, spread, hidden_raw, frames_raw, weight, bias_rows, bias,
    gate_wide, partial, edge_send, edge_recv,
    load_sem, send_sem, recv_sem, cross_send, cross_recv, turn,
):
    section = lax.axis_index("section")
    tile = lax.axis_index("tile")
    member = lax.axis_index("member")
    tiles = lax.axis_size("tile")
    place = lax.rem(tile + GRID_COLS + GRID_COLS // 2, tiles)
    grid_row, grid_col = place // GRID_COLS, lax.rem(place, GRID_COLS)
    has_up, has_down = grid_row > 0, grid_row < tiles // GRID_COLS - 1
    has_left, has_right = grid_col > 0, grid_col < GRID_COLS - 1

    def device(which, distance):
        return (which, lax.rem(tile + distance + tiles, tiles), member)

    loads = [
        pltpu.make_async_copy(hidden, hidden_raw, load_sem.at[0]),
        pltpu.make_async_copy(frames, frames_raw, load_sem.at[1]),
        pltpu.make_async_copy(biases, bias_rows, load_sem.at[2]),
        pltpu.make_async_copy(weights.at[1], weight.at[1], load_sem.at[3]),
        pltpu.make_async_copy(memory, cell, load_sem.at[4]),
        pltpu.make_async_copy(weights.at[0], weight.at[0], load_sem.at[5]),
    ]
    for load in loads:
        load.start()

    barrier = pltpu.get_barrier_semaphore()
    for distance in NEIGHBOURS:
        pl.semaphore_signal(barrier, 1, device_id=device(section, distance), device_id_type=MESH)
    depth = tile // 16
    beside = device(section, jnp.where(lax.rem(depth, 2) == 0, 16, -16))
    pl.semaphore_signal(barrier, 1, device_id=device(1 - section, 0), device_id_type=MESH)
    pl.semaphore_signal(barrier, 1, device_id=beside, device_id_type=MESH)

    def slot(index):
        return pl.ds(index * 128, 128)

    def message(step, source, target, flow, which, number):
        if number == ROW_UP:
            src = patch.at[step, 1, 1, slot(source)]
            dst = patch.at[step, 1, 9, slot(target)]
        elif number == ROW_DOWN:
            src = patch.at[step, 1, 8, slot(source)]
            dst = patch.at[step, 1, 0, slot(target)]
        else:
            src = edge_send.at[step, source, 0 if number < 5 else 1]
            dst = edge_recv.at[step, target, number - 2]
        return pltpu.make_async_remote_copy(
            src_ref=src, dst_ref=dst,
            send_sem=send_sem.at[step, flow, number], recv_sem=recv_sem.at[step, target, number],
            device_id=device(which, NEIGHBOURS[number]), device_id_type=MESH,
        )

    def messages(step, source, target, flow, which):
        return [message(step, source, target, flow, which, n) for n in range(8)]

    def cross(step):
        copies = [(edge_send.at[step, 2], edge_send.at[step, 0])]
        for first, count in CROSS:
            rows = pl.ds(first, count)
            copies.append((patch.at[step, 1, rows, slot(2)], patch.at[step, 1, rows, slot(0)]))
        return [
            pltpu.make_async_remote_copy(
                src_ref=src, dst_ref=dst, send_sem=cross_send.at[step, n], recv_sem=cross_recv.at[step, n],
                device_id=device(1, 0), device_id_type=MESH,
            )
            for n, (src, dst) in enumerate(copies)
        ]

    def lay_out(raw, step, index):
        spread[...] = raw.astype(F32)
        for y in range(8):
            patch[step, 1, 1 + y, slot(index), :] = spread[pl.ds(y, 128, stride=8), :].astype(BF16)

    row_of = lax.broadcasted_iota(jnp.int32, (8, 128), 0)
    lane_of = lax.broadcasted_iota(jnp.int32, (8, 128), 1)

    def take_edges(step, index):
        left = jnp.zeros((8, 128), F32)
        right = jnp.zeros((8, 128), F32)
        for y in range(8):
            pick = jnp.concatenate(
                [((row_of == y) & (lane_of == 0)).astype(F32), ((row_of == y) & (lane_of == 127)).astype(F32)], axis=0
            ).astype(BF16)
            both = lax.dot_general(
                pick, patch[step, 1, 1 + y, slot(index), :], (((1,), (1,)), ((), ())), preferred_element_type=F32
            )
            left += both[:8]
            right += both[8:]
        edge_send[step, index, 0] = right.astype(BF16)
        edge_send[step, index, 1] = left.astype(BF16)

    lane = lax.broadcasted_iota(jnp.int32, (128, 128), 1)

    def put(step, b, r, index, value):
        patch[step, b, r, slot(index), :] = value.astype(BF16)

    def shift(step, index):
        for r in range(1, 9):
            x = patch[step, 1, r, slot(index), :].astype(F32)
            put(step, 0, r, index, pltpu.roll(x, 1, 1))
            put(step, 2, r, index, pltpu.roll(x, 127, 1))

    def insert(step, index):
        edges = edge_recv[step, index].astype(F32).reshape(48, 128)
        edges = jnp.concatenate([edges, jnp.zeros((80, 128), F32)], axis=0).T
        for r, left_at, right_at in [(0, 15, 39), (9, 16, 40)] + [(r, r - 1, r + 23) for r in range(1, 9)]:
            live_left, live_right = has_left, has_right
            if r in (0, 9):
                live = has_up if r == 0 else has_down
                live_left, live_right = live & has_left, live & has_right
                x = jnp.where(live, patch[step, 1, r, slot(index), :].astype(F32), 0.0)
                put(step, 1, r, index, x)
                to_right, to_left = pltpu.roll(x, 1, 1), pltpu.roll(x, 127, 1)
            else:
                to_right = patch[step, 0, r, slot(index), :].astype(F32)
                to_left = patch[step, 2, r, slot(index), :].astype(F32)
            from_left = jnp.where(live_left, pltpu.roll(edges, (128 - left_at) % 128, 1), 0.0)
            from_right = jnp.where(live_right, pltpu.roll(edges, 127 - right_at, 1), 0.0)
            put(step, 0, r, index, jnp.where(lane == 0, from_left, to_right))
            put(step, 2, r, index, jnp.where(lane == 127, from_right, to_left))

    def product(step, index, pair, parts):
        chunks = [(tap, part) for tap in range(9) for part in parts]
        acc = None
        for first in range(0, len(chunks), 2):
            group = chunks[first:first + 2]
            lhs = jnp.concatenate(
                [weight[index, :, tap * 256 + part * 128:tap * 256 + part * 128 + 128] for tap, part in group], axis=1
            )
            rhs = jnp.concatenate(
                [
                    jnp.concatenate(
                        [patch[step, tap % 3, 2 * pair + r + tap // 3, slot(index + part), :] for r in range(2)], axis=1
                    )
                    for tap, part in group
                ],
                axis=0,
            )
            dot = jnp.dot(lhs, rhs, preferred_element_type=F32)
            acc = dot if acc is None else acc + dot
        return acc

    def first_half(step, index, part):
        for pair in range(4):
            offset = jnp.concatenate([bias[index]] * 2, axis=1)
            partial[index, pair] = product(step, index, pair, (part,)) + offset

    def layer(step, index, parts, pairs=(0, 3, 1, 2)):
        for pair in pairs:
            acc = product(step, index, pair, parts)
            if len(parts) == 2:
                acc += jnp.concatenate([bias[index]] * 2, axis=1)
            else:
                acc += partial[index, pair]
            for r in range(2):
                y = 2 * pair + r
                pre = acc[:, r * 128:(r + 1) * 128]
                inflow = sigmoid(pre[0:128])
                forget = sigmoid(pre[128:256])
                outflow = sigmoid(pre[256:384])
                candidate = jnp.tanh(pre[384:512])
                for n, gate in enumerate((inflow, forget, outflow, candidate)):
                    gate_wide[pl.ds(y + n * 1024, 128, stride=8), :] = gate
                old = cell[index, pl.ds(y, 128, stride=8), :]
                new = forget * old + inflow * candidate
                cell[index, pl.ds(y, 128, stride=8), :] = new
                state = outflow * jnp.tanh(new)
                if step == 0:
                    patch[1, 1, 1 + y, slot(1 + index), :] = state.astype(BF16)
                else:
                    spread[pl.ds(y, 128, stride=8), :] = state

    def finish(step, index):
        def narrow(n, carry):
            rows = pl.ds(pl.multiple_of(n * 256, 256), 256)
            gate_narrow[step, index, rows, :] = gate_wide[rows, :].astype(BF16)
            return carry

        lax.fori_loop(0, 16, narrow, 0, unroll=4)
        if step == 1:
            hidden_narrow[index] = spread[...].astype(BF16)

    def start(copies):
        for copy in copies:
            copy.start()

    def wait_recv(copies):
        for copy in copies:
            copy.wait_recv()

    def wait_send(copies):
        for copy in copies:
            copy.wait_send()

    def on(which, action):
        pl.when(section == which)(action)

    between = (depth == 1) | (depth == 2)
    inner, outer = (section == 0) & between, (section == 0) & jnp.logical_not(between)

    def hand_over(step, who):
        @pl.when(who)
        def _():
            start(cross(step))

    def pass_turn(who, copies):
        @pl.when(who)
        def _():
            wait_send(copies)
            pl.semaphore_signal(turn, 1, device_id=beside, device_id_type=MESH)

    def take_turn(who, copies):
        @pl.when(who)
        def _():
            pl.semaphore_wait(turn, 1)
            start(copies)

    with phase("load"):
        loads[0].wait()
    with phase("lay"):
        for index in range(2):
            lay_out(hidden_raw[index], 0, 1 + index)
            take_edges(0, 1 + index)
    with phase("framesprep"):
        loads[1].wait()

        @pl.when(section == 0)
        def _():
            for step in range(2):
                lay_out(frames_raw[step], step, 0)
                take_edges(step, 0)
                shift(step, 0)

    with phase("barrier"):
        pl.semaphore_wait(barrier, 10)
    with phase("send0"):
        start(messages(0, 2, 2, 2, section))
        start(messages(0, 1, 1, 1, section))

        @pl.when(section == 0)
        def _():
            start(messages(0, 0, 0, 0, section))

        hand_over(0, outer)

    with phase("shift0"):
        shift(0, 2)
        shift(0, 1)
    with phase("bias"):
        loads[2].wait()
        rows = jnp.concatenate([bias_rows[n // 4:n // 4 + 1, (n % 4) * 128:(n % 4 + 1) * 128] for n in range(8)], axis=0)
        columns = jnp.concatenate([rows, jnp.zeros((120, 128), F32)], axis=0).T
        for n in range(8):
            bias[n // 4, (n % 4) * 128:(n % 4 + 1) * 128, :] = jnp.broadcast_to(columns[:, n:n + 1], (128, 128))

    def take_in(step, index, first=0):
        with phase(f"wait_halo_s{step}_{index}"):
            wait_recv(messages(step, index, index, index, section)[first:])
        with phase(f"insert_s{step}_{index}"):
            insert(step, index)

    def pass_on(step, who):
        with phase(f"pass_on_s{step}"):
            @pl.when((section == 1) & who)
            def _():
                wait_recv(cross(step)[:3])
                start(messages(step, 0, 0, 0, section))

    def rest(step):
        with phase(f"wait_rest_s{step}"):
            @pl.when(section == 1)
            def _():
                wait_recv(cross(step)[3:])
                shift(step, 0)

    take_in(0, 2)
    take_in(0, 1)
    with phase("turn0"):
        pass_turn(outer, cross(0))
        take_turn(inner, cross(0))
    with phase("wait_w"):
        for n in (3, 4, 5):
            loads[n].wait()
    with phase("layer_s0_1"):
        layer(0, 1, (0, 1), (0, 3))
        start(messages(1, 2, 2, 2, section)[:2])
        layer(0, 1, (0, 1), (1, 2))
    with phase("send1"):
        take_edges(1, 2)
        start(messages(1, 2, 2, 2, section)[2:])

        @pl.when(section == 0)
        def _():
            start(messages(1, 0, 0, 0, section))

    pass_on(0, jnp.logical_not(between))
    with phase("finish_s0_1"):
        finish(0, 1)
        shift(1, 2)
    with phase("half_s0_0"):
        first_half(0, 0, 1)
    pass_on(0, between)
    rest(0)
    take_in(0, 0)
    with phase("layer_s0_0"):
        layer(0, 0, (0,), (0, 3))
        start(messages(1, 1, 1, 1, section)[:2])
        layer(0, 0, (0,), (1, 2))
    with phase("send2"):
        take_edges(1, 1)
        start(messages(1, 1, 1, 1, section)[2:])
        hand_over(1, inner)

    with phase("finish_s0_0"):
        finish(0, 0)
        shift(1, 1)
    pass_on(1, between)
    take_in(1, 2)
    with phase("half_s1_1"):
        first_half(1, 1, 1)
    with phase("turn1"):
        pass_turn(inner, cross(0) + cross(1))
        take_turn(outer, cross(1))
    pass_on(1, jnp.logical_not(between))
    take_in(1, 1)
    with phase("layer_s1_1"):
        layer(1, 1, (0,))
    with phase("half_s1_0"):
        first_half(1, 0, 1)
    with phase("finish_s1_1"):
        finish(1, 1)
    rest(1)
    take_in(1, 0)
    with phase("layer_s1_0"):
        layer(1, 0, (0,))
    with phase("finish_s1_0"):
        finish(1, 0)

    for step in range(2):
        for index in range(3):
            wait_send(messages(step, index, index, index, section))

    @pl.when(outer)
    def _():
        wait_send(cross(1))


def write_out(*refs):
    sources, targets, sem = refs[:3], refs[3:6], refs[6]
    copies = [pltpu.make_async_copy(src, dst, sem.at[n]) for n, (src, dst) in enumerate(zip(sources, targets))]
    for copy in copies:
        copy.start()
    for copy in copies:
        copy.wait()


def body(frames, hidden_init, memory_init, weights, biases):
    frames = frames.reshape(2, 1024, 128)
    hidden_init = hidden_init.reshape(2, 1024, 128)
    memory_init = memory_init.reshape(2, 1024, 128)
    vmem = pltpu.VMEM
    dma = pltpu.SemaphoreType.DMA
    shapes = (
        jax.ShapeDtypeStruct((2, 1024, 128), BF16),
        jax.ShapeDtypeStruct((2, 1024, 128), F32),
        jax.ShapeDtypeStruct((2, 2, 4096, 128), BF16),
    )
    results = pl.pallas_call(
        kernel,
        out_shape=shapes,
        in_specs=[pl.BlockSpec(memory_space=pltpu.HBM)] * 5,
        out_specs=[pl.BlockSpec(memory_space=pltpu.VMEM)] * 3,
        scratch_shapes=[
            vmem((2, 3, 10, 384, 128), BF16),
            vmem((1024, 128), F32),
            vmem((2, 1024, 128), BF16),
            vmem((2, 1024, 128), BF16),
            vmem((2, 512, 2304), BF16),
            vmem((2, 512), F32),
            vmem((2, 512, 128), F32),
            vmem((4096, 128), F32),
            vmem((2, 4, 512, 256), F32),
            vmem((2, 3, 2, 8, 128), BF16),
            vmem((2, 3, 6, 8, 128), BF16),
            dma((6,)),
            dma((2, 3, 8)),
            dma((2, 3, 8)),
            dma((2, 1 + len(CROSS))),
            dma((2, 1 + len(CROSS))),
            pltpu.SemaphoreType.REGULAR,
        ],
        compiler_params=pltpu.CompilerParams(
            collective_id=0, has_side_effects=True, vmem_limit_bytes=32 << 20
        ),
        name="wavefront",
    )(*[pltpu.with_memory_space_constraint(x, pltpu.HBM) for x in (frames, hidden_init, memory_init, weights, biases)])
    hidden_out, memory_out, gates_out = pl.pallas_call(
        write_out,
        out_shape=shapes,
        in_specs=[pl.BlockSpec(memory_space=pl.ANY)] * 3,
        out_specs=[pl.BlockSpec(memory_space=pltpu.HBM)] * 3,
        scratch_shapes=[dma((3,))],
        compiler_params=pltpu.CompilerParams(vmem_limit_bytes=1 << 20),
        name="write_out",
    )(*results)
    return (
        hidden_out.reshape(2, 1, 128, 8, 128),
        memory_out.reshape(2, 1, 128, 8, 128),
        gates_out.reshape(2, 2, 1, 512, 8, 128),
    )


def solution(mesh):
    states = P("section", ("member", "tile"), None, None, None)
    in_specs = (
        P(None, ("member", "tile"), None, None, None),
        states,
        states,
        P("section", None, None),
        P("section", None),
    )
    out_specs = (states, states, P(None, "section", ("member", "tile"), None, None, None))
    return jax.shard_map(body, mesh=mesh, in_specs=in_specs, out_specs=out_specs, check_vma=False)
```

```python
import contextlib

import jax
import jax.numpy as jnp
from jax import lax
from jax.experimental import pallas as pl
from jax.experimental.pallas import tpu as pltpu
from jax.sharding import PartitionSpec as P

GRID_COLS = 8
MESH = pl.DeviceIdType.MESH
F32 = jnp.float32
BF16 = jnp.bfloat16

ROW_UP, ROW_DOWN = 0, 1
NEIGHBOURS = (-8, 8, 1, 9, -7, -1, 7, -9)
CROSS = tuple((row, 1) for row in (1, 8, 2, 3, 4, 5, 6, 7))


def phase(name):
    return contextlib.nullcontext()


def sigmoid(x):
    return 0.5 * jnp.tanh(0.5 * x) + 0.5


def products(weight, rows_of, pair, parts):
    chunks = [(tap, part) for tap in range(9) for part in parts]
    acc = None
    for first in range(0, len(chunks), 2):
        group = chunks[first:first + 2]
        lhs = jnp.concatenate(
            [weight[:, tap * 256 + part * 128:tap * 256 + part * 128 + 128] for tap, part in group], axis=1
        )
        rhs = jnp.concatenate(
            [jnp.concatenate([rows_of(tap, part, 2 * pair + r) for r in range(2)], axis=1) for tap, part in group],
            axis=0,
        )
        dot = jnp.dot(lhs, rhs, preferred_element_type=F32)
        acc = dot if acc is None else acc + dot
    return acc


def advance(pre, old):
    inflow = sigmoid(pre[0:128])
    forget = sigmoid(pre[128:256])
    outflow = sigmoid(pre[256:384])
    candidate = jnp.tanh(pre[384:512])
    new = forget * old + inflow * candidate
    return (inflow, forget, outflow, candidate), new, outflow * jnp.tanh(new)


def spread_gates(gate_wide, y, gates):
    for n, gate in enumerate(gates):
        gate_wide[pl.ds(y + n * 1024, 128, stride=8), :] = gate


def kernel(
    frames, hidden, memory, weights, biases,
    gate_narrow, hidden_narrow, cell, window, partial_first, weight_first,
    patch, spread, hidden_raw, frames_raw, weight_second, bias_rows, bias,
    gate_wide, partial_second, edge_send, edge_recv,
    load_sem, send_sem, recv_sem, cross_send, cross_recv, turn,
):
    weight, partial = (weight_first, weight_second), (partial_first, partial_second)
    section = lax.axis_index("section")
    tile = lax.axis_index("tile")
    member = lax.axis_index("member")
    tiles = lax.axis_size("tile")
    place = lax.rem(tile + GRID_COLS + GRID_COLS // 2, tiles)
    grid_row, grid_col = place // GRID_COLS, lax.rem(place, GRID_COLS)
    has_up, has_down = grid_row > 0, grid_row < tiles // GRID_COLS - 1
    has_left, has_right = grid_col > 0, grid_col < GRID_COLS - 1

    def device(which, distance):
        return (which, lax.rem(tile + distance + tiles, tiles), member)

    loads = [
        pltpu.make_async_copy(hidden, hidden_raw, load_sem.at[0]),
        pltpu.make_async_copy(frames, frames_raw, load_sem.at[1]),
        pltpu.make_async_copy(biases, bias_rows, load_sem.at[2]),
        pltpu.make_async_copy(weights.at[1], weight[1], load_sem.at[3]),
        pltpu.make_async_copy(memory, cell, load_sem.at[4]),
        pltpu.make_async_copy(weights.at[0], weight[0], load_sem.at[5]),
    ]
    for load in loads:
        load.start()

    barrier = pltpu.get_barrier_semaphore()
    for distance in NEIGHBOURS:
        pl.semaphore_signal(barrier, 1, device_id=device(section, distance), device_id_type=MESH)
    depth = tile // 16
    beside = device(section, jnp.where(lax.rem(depth, 2) == 0, 16, -16))
    pl.semaphore_signal(barrier, 1, device_id=device(1 - section, 0), device_id_type=MESH)
    pl.semaphore_signal(barrier, 1, device_id=beside, device_id_type=MESH)

    def slot(index):
        return pl.ds(index * 128, 128)

    def message(step, source, target, flow, which, number):
        if number == ROW_UP:
            src = patch.at[step, 1, 1, slot(source)]
            dst = patch.at[step, 1, 9, slot(target)]
        elif number == ROW_DOWN:
            src = patch.at[step, 1, 8, slot(source)]
            dst = patch.at[step, 1, 0, slot(target)]
        else:
            src = edge_send.at[step, source, 0 if number < 5 else 1]
            dst = edge_recv.at[step, target, number - 2]
        return pltpu.make_async_remote_copy(
            src_ref=src, dst_ref=dst,
            send_sem=send_sem.at[step, flow, number], recv_sem=recv_sem.at[step, target, number],
            device_id=device(which, NEIGHBOURS[number]), device_id_type=MESH,
        )

    def messages(step, source, target, flow, which):
        return [message(step, source, target, flow, which, n) for n in range(8)]

    def cross(step):
        copies = [(edge_send.at[step, 2], edge_send.at[step, 0])]
        for first, count in CROSS:
            rows = pl.ds(first, count)
            copies.append((patch.at[step, 1, rows, slot(2)], patch.at[step, 1, rows, slot(0)]))
        return [
            pltpu.make_async_remote_copy(
                src_ref=src, dst_ref=dst, send_sem=cross_send.at[step, n], recv_sem=cross_recv.at[step, n],
                device_id=device(1, 0), device_id_type=MESH,
            )
            for n, (src, dst) in enumerate(copies)
        ]

    def lay_out(raw, step, index):
        spread[...] = raw.astype(F32)
        for y in range(8):
            patch[step, 1, 1 + y, slot(index), :] = spread[pl.ds(y, 128, stride=8), :].astype(BF16)

    row_of = lax.broadcasted_iota(jnp.int32, (8, 128), 0)
    lane_of = lax.broadcasted_iota(jnp.int32, (8, 128), 1)

    def take_edges(step, index):
        left = jnp.zeros((8, 128), F32)
        right = jnp.zeros((8, 128), F32)
        for y in range(8):
            pick = jnp.concatenate(
                [((row_of == y) & (lane_of == 0)).astype(F32), ((row_of == y) & (lane_of == 127)).astype(F32)], axis=0
            ).astype(BF16)
            both = lax.dot_general(
                pick, patch[step, 1, 1 + y, slot(index), :], (((1,), (1,)), ((), ())), preferred_element_type=F32
            )
            left += both[:8]
            right += both[8:]
        edge_send[step, index, 0] = right.astype(BF16)
        edge_send[step, index, 1] = left.astype(BF16)

    lane = lax.broadcasted_iota(jnp.int32, (128, 128), 1)

    def put(step, b, r, index, value):
        patch[step, b, r, slot(index), :] = value.astype(BF16)

    def shift(step, index):
        for r in range(1, 9):
            x = patch[step, 1, r, slot(index), :].astype(F32)
            put(step, 0, r, index, pltpu.roll(x, 1, 1))
            put(step, 2, r, index, pltpu.roll(x, 127, 1))

    def insert(step, index):
        edges = edge_recv[step, index].astype(F32).reshape(48, 128)
        edges = jnp.concatenate([edges, jnp.zeros((80, 128), F32)], axis=0).T
        for r, left_at, right_at in [(0, 15, 39), (9, 16, 40)] + [(r, r - 1, r + 23) for r in range(1, 9)]:
            live_left, live_right = has_left, has_right
            if r in (0, 9):
                live = has_up if r == 0 else has_down
                live_left, live_right = live & has_left, live & has_right
                x = jnp.where(live, patch[step, 1, r, slot(index), :].astype(F32), 0.0)
                put(step, 1, r, index, x)
                to_right, to_left = pltpu.roll(x, 1, 1), pltpu.roll(x, 127, 1)
            else:
                to_right = patch[step, 0, r, slot(index), :].astype(F32)
                to_left = patch[step, 2, r, slot(index), :].astype(F32)
            from_left = jnp.where(live_left, pltpu.roll(edges, (128 - left_at) % 128, 1), 0.0)
            from_right = jnp.where(live_right, pltpu.roll(edges, 127 - right_at, 1), 0.0)
            put(step, 0, r, index, jnp.where(lane == 0, from_left, to_right))
            put(step, 2, r, index, jnp.where(lane == 127, from_right, to_left))

    def product(step, index, pair, parts):
        return products(
            weight[index], lambda tap, part, y: patch[step, tap % 3, y + tap // 3, slot(index + part), :], pair, parts
        )

    def first_half(step, index, part):
        for pair in range(4):
            offset = jnp.concatenate([bias[index]] * 2, axis=1)
            partial[index][pair] = product(step, index, pair, (part,)) + offset

    def layer(step, index, parts, pairs=(0, 3, 1, 2)):
        for pair in pairs:
            acc = product(step, index, pair, parts)
            if len(parts) == 2:
                acc += jnp.concatenate([bias[index]] * 2, axis=1)
            else:
                acc += partial[index][pair]
            for r in range(2):
                y = 2 * pair + r
                old = cell[index, pl.ds(y, 128, stride=8), :]
                gates, new, state = advance(acc[:, r * 128:(r + 1) * 128], old)
                spread_gates(gate_wide, y, gates)
                cell[index, pl.ds(y, 128, stride=8), :] = new
                if step == 0:
                    patch[1, 1, 1 + y, slot(1 + index), :] = state.astype(BF16)
                else:
                    spread[pl.ds(y, 128, stride=8), :] = state

    def finish(step, index):
        def narrow(n, carry):
            rows = pl.ds(pl.multiple_of(n * 256, 256), 256)
            gate_narrow[2 * step + index * (1 - step), rows, :] = gate_wide[rows, :].astype(BF16)
            return carry

        lax.fori_loop(0, 16, narrow, 0, unroll=4)
        if step == 1:
            hidden_narrow[...] = spread[...].astype(BF16)

    def start(copies):
        for copy in copies:
            copy.start()

    def wait_recv(copies):
        for copy in copies:
            copy.wait_recv()

    def wait_send(copies):
        for copy in copies:
            copy.wait_send()

    def on(which, action):
        pl.when(section == which)(action)

    between = (depth == 1) | (depth == 2)
    inner, outer = (section == 0) & between, (section == 0) & jnp.logical_not(between)

    def hand_over(step, who):
        @pl.when(who)
        def _():
            start(cross(step))

    def pass_turn(who, copies):
        @pl.when(who)
        def _():
            wait_send(copies)
            pl.semaphore_signal(turn, 1, device_id=beside, device_id_type=MESH)

    def take_turn(who, copies):
        @pl.when(who)
        def _():
            pl.semaphore_wait(turn, 1)
            start(copies)

    with phase("load"):
        loads[0].wait()
    with phase("lay"):
        for index in range(2):
            lay_out(hidden_raw[index], 0, 1 + index)
            take_edges(0, 1 + index)
    with phase("framesprep"):
        loads[1].wait()

        @pl.when(section == 0)
        def _():
            for step in range(2):
                lay_out(frames_raw[step], step, 0)
                take_edges(step, 0)
                shift(step, 0)

    with phase("barrier"):
        pl.semaphore_wait(barrier, 10)
    with phase("send0"):
        start(messages(0, 2, 2, 2, section))
        start(messages(0, 1, 1, 1, section))

        @pl.when(section == 0)
        def _():
            start(messages(0, 0, 0, 0, section))

        hand_over(0, outer)

    with phase("shift0"):
        shift(0, 2)
        shift(0, 1)
    with phase("bias"):
        loads[2].wait()
        rows = jnp.concatenate([bias_rows[n // 4:n // 4 + 1, (n % 4) * 128:(n % 4 + 1) * 128] for n in range(8)], axis=0)
        columns = jnp.concatenate([rows, jnp.zeros((120, 128), F32)], axis=0).T
        for n in range(8):
            bias[n // 4, (n % 4) * 128:(n % 4 + 1) * 128, :] = jnp.broadcast_to(columns[:, n:n + 1], (128, 128))

    def take_in(step, index, first=0):
        with phase(f"wait_halo_s{step}_{index}"):
            wait_recv(messages(step, index, index, index, section)[first:])
        with phase(f"insert_s{step}_{index}"):
            insert(step, index)

    def pass_on(step, who):
        with phase(f"pass_on_s{step}"):
            @pl.when((section == 1) & who)
            def _():
                wait_recv(cross(step)[:3])
                start(messages(step, 0, 0, 0, section))

    def rest(step):
        with phase(f"wait_rest_s{step}"):
            @pl.when(section == 1)
            def _():
                wait_recv(cross(step)[3:])
                shift(step, 0)

    with phase("turn0"):
        pass_turn(outer, cross(0))
    take_in(0, 2)
    with phase("turn0b"):
        take_turn(inner, cross(0))
    take_in(0, 1)
    with phase("wait_w"):
        for n in (3, 4, 5):
            loads[n].wait()
    with phase("layer_s0_1"):
        layer(0, 1, (0, 1), (0, 3))
        start(messages(1, 2, 2, 2, section)[:2])
        layer(0, 1, (0, 1), (1, 2))
    with phase("send1"):
        take_edges(1, 2)
        start(messages(1, 2, 2, 2, section)[2:])

        @pl.when(section == 0)
        def _():
            start(messages(1, 0, 0, 0, section))

    pass_on(0, jnp.logical_not(between))
    with phase("finish_s0_1"):
        finish(0, 1)
        shift(1, 2)
    with phase("half_s0_0"):
        first_half(0, 0, 1)
    pass_on(0, between)
    rest(0)
    take_in(0, 0)
    with phase("layer_s0_0"):
        layer(0, 0, (0,), (0, 3))
        start(messages(1, 1, 1, 1, section)[:2])
        layer(0, 0, (0,), (1, 2))
    with phase("send2"):
        take_edges(1, 1)
        start(messages(1, 1, 1, 1, section)[2:])
        hand_over(1, inner)

    with phase("finish_s0_0"):
        finish(0, 0)
        shift(1, 1)
    pass_on(1, between)
    take_in(1, 2)
    with phase("half_s1_1"):
        first_half(1, 1, 1)
    with phase("turn1"):
        pass_turn(inner, cross(0) + cross(1))
        take_turn(outer, cross(1))
    pass_on(1, jnp.logical_not(between))
    take_in(1, 1)
    with phase("layer_s1_1"):
        layer(1, 1, (0,))
    with phase("half_s1_0"):
        first_half(1, 0, 1)
    with phase("finish_s1_1"):
        finish(1, 1)
    rest(1)
    take_in(1, 0)
    with phase("finish_s1_0"):
        for b in range(3):
            for r in range(10):
                window[b, r] = patch[1, b, r, slot(0), :]

    for step in range(2):
        for index in range(3):
            wait_send(messages(step, index, index, index, section))

    @pl.when(outer)
    def _():
        wait_send(cross(1))


def last_layer(
    gates, hidden_second, memory, window, partial, weight,
    hidden_out, memory_out, gates_out,
    gate_wide, gate_narrow, spread, hidden_narrow, cell, sem,
):
    def write(n, src, dst):
        return pltpu.make_async_copy(src, dst, sem.at[n])

    early = [
        write(0, gates.at[0], gates_out.at[0, 0]),
        write(1, gates.at[1], gates_out.at[0, 1]),
        write(2, gates.at[2], gates_out.at[1, 1]),
        write(3, hidden_second, hidden_out.at[1]),
        write(4, memory.at[1], memory_out.at[1]),
    ]
    for copy in early:
        copy.start()
    for pair in range(4):
        acc = products(weight, lambda tap, part, y: window[tap % 3, y + tap // 3], pair, (0,)) + partial[pair]
        for r in range(2):
            y = 2 * pair + r
            values, new, state = advance(acc[:, r * 128:(r + 1) * 128], memory[0, pl.ds(y, 128, stride=8), :])
            spread_gates(gate_wide, y, values)
            cell[pl.ds(y, 128, stride=8), :] = new
            spread[pl.ds(y, 128, stride=8), :] = state
    late = [write(5, cell, memory_out.at[0])]
    late[0].start()
    for n in range(4):
        rows = pl.ds(n * 1024, 1024)
        gate_narrow[rows, :] = gate_wide[rows, :].astype(BF16)
        late.append(write(6 + n, gate_narrow.at[rows], gates_out.at[1, 0, rows]))
        late[-1].start()
    hidden_narrow[...] = spread[...].astype(BF16)
    late.append(write(10, hidden_narrow, hidden_out.at[0]))
    late[-1].start()
    for copy in early + late:
        copy.wait()


def body(frames, hidden_init, memory_init, weights, biases):
    frames = frames.reshape(2, 1024, 128)
    hidden_init = hidden_init.reshape(2, 1024, 128)
    memory_init = memory_init.reshape(2, 1024, 128)
    vmem = pltpu.VMEM
    dma = pltpu.SemaphoreType.DMA
    shapes = (
        jax.ShapeDtypeStruct((2, 1024, 128), BF16),
        jax.ShapeDtypeStruct((2, 1024, 128), F32),
        jax.ShapeDtypeStruct((2, 2, 4096, 128), BF16),
    )
    results = pl.pallas_call(
        kernel,
        out_shape=(
            jax.ShapeDtypeStruct((3, 4096, 128), BF16),
            jax.ShapeDtypeStruct((1024, 128), BF16),
            jax.ShapeDtypeStruct((2, 1024, 128), F32),
            jax.ShapeDtypeStruct((3, 10, 128, 128), BF16),
            jax.ShapeDtypeStruct((4, 512, 256), F32),
            jax.ShapeDtypeStruct((512, 2304), BF16),
        ),
        in_specs=[pl.BlockSpec(memory_space=pltpu.HBM)] * 5,
        out_specs=[pl.BlockSpec(memory_space=pltpu.VMEM)] * 6,
        scratch_shapes=[
            vmem((2, 3, 10, 384, 128), BF16),
            vmem((1024, 128), F32),
            vmem((2, 1024, 128), BF16),
            vmem((2, 1024, 128), BF16),
            vmem((512, 2304), BF16),
            vmem((2, 512), F32),
            vmem((2, 512, 128), F32),
            vmem((4096, 128), F32),
            vmem((4, 512, 256), F32),
            vmem((2, 3, 2, 8, 128), BF16),
            vmem((2, 3, 6, 8, 128), BF16),
            dma((6,)),
            dma((2, 3, 8)),
            dma((2, 3, 8)),
            dma((2, 1 + len(CROSS))),
            dma((2, 1 + len(CROSS))),
            pltpu.SemaphoreType.REGULAR,
        ],
        compiler_params=pltpu.CompilerParams(
            collective_id=0, has_side_effects=True, vmem_limit_bytes=32 << 20
        ),
        name="wavefront",
    )(*[pltpu.with_memory_space_constraint(x, pltpu.HBM) for x in (frames, hidden_init, memory_init, weights, biases)])
    hidden_out, memory_out, gates_out = pl.pallas_call(
        last_layer,
        out_shape=shapes,
        in_specs=[pl.BlockSpec(memory_space=pltpu.VMEM)] * 6,
        out_specs=[pl.BlockSpec(memory_space=pltpu.HBM)] * 3,
        scratch_shapes=[
            vmem((4096, 128), F32),
            vmem((4096, 128), BF16),
            vmem((1024, 128), F32),
            vmem((1024, 128), BF16),
            vmem((1024, 128), F32),
            dma((11,)),
        ],
        compiler_params=pltpu.CompilerParams(vmem_limit_bytes=24 << 20),
        name="last_layer",
    )(*results)
    return (
        hidden_out.reshape(2, 1, 128, 8, 128),
        memory_out.reshape(2, 1, 128, 8, 128),
        gates_out.reshape(2, 2, 1, 512, 8, 128),
    )


def solution(mesh):
    states = P("section", ("member", "tile"), None, None, None)
    in_specs = (
        P(None, ("member", "tile"), None, None, None),
        states,
        states,
        P("section", None, None),
        P("section", None),
    )
    out_specs = (states, states, P(None, "section", ("member", "tile"), None, None, None))
    return jax.shard_map(body, mesh=mesh, in_specs=in_specs, out_specs=out_specs, check_vma=False)
```
